32 devices in a mesh: gx: 2 (over x), gy: 4 (over y, core), gz: 4 (over z).
Axes of the slice: x: 2, y: 2, z: 4, core: 2. Of those that a mesh axis runs over, the one named last changes fastest.
Arguments:
- displacement: float32 [3, 16, 32, 512], P(None, 'gx', 'gz', 'gy'), may hold values from -0.1 to 0.1
- velocity: float32 [3, 16, 32, 512], P(None, 'gx', 'gz', 'gy'), may hold values from -0.4 to 0.4
- body_force: float32 [3, 16, 32, 512], P(None, 'gx', 'gz', 'gy'), may hold values from -4 to 4
- broken: int32 [12, 16, 32, 512], P(None, 'gx', 'gz', 'gy'), may hold values from 0 to 1073741823
Outputs:
- new_displacement: float32 [3, 16, 32, 512], P(None, 'gx', 'gz', 'gy')
- new_velocity: float32 [3, 16, 32, 512], P(None, 'gx', 'gz', 'gy')
- new_acceleration: float32 [3, 16, 32, 512], P(None, 'gx', 'gz', 'gy')
- strain_energy: float32 [], replicated
The draws below stay inside these ranges and needn't reach their ends.
All inputs are finite; a program needn't handle non-finite values.
Results may differ from the reference program's by a relative error of at most 0.0003.
Values sent between devices are 32-bit elements; how exact they have to be, the bound alone decides.
A program may use at most 128 MiB of HBM per device.

```python
import math
import jax
import jax.numpy as jnp
from jax import lax

CX = 8
WORDS = 12
NX = 16
NZ = 32
NY = 512


def draw_displacement(key, part):
    key_noise = jax.random.fold_in(key, 11)
    along_x = (jnp.arange(NX, dtype=jnp.float32) + 0.5) / NX
    noise = jax.random.normal(key_noise, (3, NX, NZ, NY), jnp.float32)
    values = noise * (0.03 * (0.5 + along_x))[None, :, None, None]
    return jnp.clip(values, -0.1, 0.1)


def place_ends(result, own_key, low, high):
    longest = result.shape.index(max(result.shape))
    spots = []
    for shift in (0, 1):
        where = [jax.random.randint(jax.random.fold_in(own_key, axis), (), 0, length) for axis, length in enumerate(result.shape)]
        where[longest] = (where[longest] + shift) % result.shape[longest]
        spots.append(tuple(where))
    return result.at[spots[0]].set(low).at[spots[1]].set(high)


def block_levels(own_key, dims, split, least, high):
    factor_of, own = 1.0, jax.random.fold_in(own_key, 6)
    for axis_at, blocks in split:
        heights = jnp.exp(jax.random.uniform(jax.random.fold_in(own, axis_at), (blocks,), jnp.float32, least / len(split), high / len(split)))
        factor_of = factor_of * jnp.repeat(heights, dims[axis_at] // blocks).reshape([-1 if axis == axis_at else 1 for axis in range(len(dims))])
    return factor_of


def bell_draw(own_key, shape, width, most, split=(), held_as=jnp.bfloat16):
    entries = jax.random.normal(own_key, shape, jnp.float32) * width
    if len(split) > 0:
        entries = block_levels(own_key, shape, split, -0.22, 0.18) * entries
    return jnp.clip(entries, min=-most, max=most).astype(held_as)


def setup_inputs(seed: int = 0) -> dict:
    seeds = jax.random.split(jax.random.key(seed), 5)
    displacement = draw_displacement(jax.random.fold_in(seeds[4], 71), 0)
    velocity = bell_draw(seeds[1], (3, NX, NZ, NY), 0.15, 0.4, ((1, 2), (2, 4), (3, 4)), jnp.float32)
    body_force = bell_draw(seeds[2], (3, NX, NZ, NY), 1.0, 4.0, ((1, 2), (2, 4), (3, 4)), jnp.float32)
    broken = place_ends(jax.random.randint(seeds[3], (WORDS, NX, NZ, NY), 0, 1073741824), jax.random.fold_in(seeds[3], 1), 0, 1073741823).astype(jnp.int32)
    return dict(displacement=displacement, velocity=velocity, body_force=body_force, broken=broken)


TIME_STEP = 0.05
MICRO_MODULUS = 4.0
BITS_PER_WORD = 30
OFFSET_LIST = tuple(((step_x, step_z, step_y) for step_x in range(-3, 4) for step_z in range(-3, 4) for step_y in range(-3, 4) if (step_x, step_z, step_y) != (0, 0, 0)))

def bond_sum(extended, mask_block, depth_start, depth_total, row_count, depth_count, width_count, with_energy):
    center = extended[:, 3:3 + row_count, 3:3 + depth_count, 3:3 + width_count]
    depth_index = depth_start + jnp.arange(depth_count, dtype=jnp.int32)
    force_x = jnp.zeros(center.shape[1:], jnp.float32)
    force_z = jnp.zeros(center.shape[1:], jnp.float32)
    force_y = jnp.zeros(center.shape[1:], jnp.float32)
    energy = jnp.zeros(center.shape[1:], jnp.float32)
    for bond_index, (step_x, step_z, step_y) in enumerate(OFFSET_LIST):
        neighbour = extended[:, 3 + step_x:3 + step_x + row_count, 3 + step_z:3 + step_z + depth_count, 3 + step_y:3 + step_y + width_count]
        relative = neighbour - center
        bond_x = relative[0] + step_x
        bond_z = relative[1] + step_z
        bond_y = relative[2] + step_y
        length = jnp.sqrt(bond_x * bond_x + bond_z * bond_z + bond_y * bond_y)
        rest_length = math.sqrt(step_x * step_x + step_z * step_z + step_y * step_y)
        influence = math.exp(-rest_length * rest_length / 9.0)
        stretch = (length - rest_length) / rest_length
        broken_bit = jnp.right_shift(mask_block[bond_index // BITS_PER_WORD], bond_index % BITS_PER_WORD) & 1
        inside = (depth_index + step_z >= 0) & (depth_index + step_z < depth_total)
        intact = jnp.where(inside[None, :, None], 1 - broken_bit, 0).astype(jnp.float32)
        factor = intact * (MICRO_MODULUS * influence) * stretch / length
        force_x = force_x + factor * bond_x
        force_z = force_z + factor * bond_z
        force_y = force_y + factor * bond_y
        if with_energy:
            energy = energy + intact * (0.25 * MICRO_MODULUS * influence * rest_length) * stretch * stretch
    return (jnp.stack([force_x, force_z, force_y]), jnp.sum(energy))

def slab_forces(field_in, broken, with_energy):
    padded = jnp.pad(field_in, ((0, 0), (3, 3), (3, 3), (3, 3)), mode='wrap')
    starts = jnp.arange(NX // CX, dtype=jnp.int32) * CX

    def block_force(first_row):
        first_row = first_row.astype(jnp.int32)
        anchor = jnp.zeros((), jnp.int32)
        extended = lax.dynamic_slice(padded, (anchor, first_row, anchor, anchor), (3, CX + 6, NZ + 6, NY + 6))
        mask_block = lax.dynamic_slice(broken, (anchor, first_row, anchor, anchor), (WORDS, CX, NZ, NY))
        return bond_sum(extended, mask_block, 0, NZ, CX, NZ, NY, with_energy)
    pieces, energies = lax.map(block_force, starts)
    forces = jnp.moveaxis(pieces, 0, 1).reshape(3, NX, NZ, NY)
    return (forces, jnp.sum(energies))

def reference(displacement, velocity, body_force, broken):
    first_force, unused = slab_forces(displacement, broken, False)
    first_acceleration = first_force + body_force
    new_displacement = displacement + TIME_STEP * velocity + 0.5 * TIME_STEP * TIME_STEP * first_acceleration
    second_force, energy = slab_forces(new_displacement, broken, True)
    new_acceleration = second_force + body_force
    new_velocity = velocity + 0.5 * TIME_STEP * (first_acceleration + new_acceleration)
    strain_energy = energy / jnp.float32(NX * NY)
    return (new_displacement, new_velocity, new_acceleration, strain_energy)
```

```python
import functools
import math

import jax
import jax.numpy as jnp
from jax import lax
from jax.experimental import pallas as pl
from jax.experimental.pallas import tpu as pltpu
from jax.sharding import PartitionSpec as P

TIME_STEP = 0.05
MICRO_MODULUS = 4.0
BITS_PER_WORD = 30
W = 3
REACH = range(-W, W + 1)
BONDS = tuple(
    (p, q, r) for p in REACH for q in REACH for r in REACH if (p, q, r) != (0, 0, 0)
)
INDEX = {bond: k for k, bond in enumerate(BONDS)}
WORD_COUNT = -(-len(BONDS) // BITS_PER_WORD)
AXES = ("gx", "gy", "gz")
MESH = pl.DeviceIdType.MESH
HIGH, LOW = 0, 1
SIDES = (-1, 1)


def align(n):
    return -(-n // 8) * 8


def depth_bits(shape, depth_start, depth_total):
    depth = lax.broadcasted_iota(jnp.int32, shape, 0) + depth_start
    words = [jnp.zeros(shape, jnp.int32) for _ in range(WORD_COUNT)]
    for q in REACH:
        if q == 0:
            continue
        outside = (depth + q < 0) | (depth + q >= depth_total)
        for w in range(WORD_COUNT):
            bits = 0
            for (p, q2, r), k in INDEX.items():
                if q2 == q and k // BITS_PER_WORD == w:
                    bits |= 1 << (k % BITS_PER_WORD)
            if bits:
                words[w] = words[w] | jnp.where(outside, bits, 0)
    return words


def store_masks(broken_ref, mask_ref, outside_ref, depth_start, depth_total):
    rows = broken_ref.shape[1]
    for w, word in enumerate(depth_bits(broken_ref.shape[2:], depth_start, depth_total)):
        outside_ref[w] = word

    def body(x, carry):
        for w in range(WORD_COUNT):
            word = broken_ref[w, x] | outside_ref[w]
            for k in range(w * BITS_PER_WORD, min(len(BONDS), (w + 1) * BITS_PER_WORD)):
                p, q, r = BONDS[k]
                weight = MICRO_MODULUS * math.exp(-(p * p + q * q + r * r) / 9.0)
                bit = word & (1 << (k % BITS_PER_WORD))
                mask_ref[k, x] = jnp.where(bit == 0, jnp.float32(weight), jnp.float32(0.0))
        return carry

    lax.fori_loop(0, rows, body, 0)


def row_bonds(p, x, e_ref, mask_ref, acc_ref, depth, energy):
    center = [e_ref[W, c, x + W, W : W + depth] for c in range(3)]
    force = [acc_ref[c, x] for c in range(3)]
    center_x = center[0] - float(p)
    center_z = {q: center[1] - float(q) for q in REACH}
    classes = {}
    for q in REACH:
        for r in REACH:
            if (p, q, r) != (0, 0, 0):
                key = 0 if energy is None else q * q + r * r
                classes.setdefault(key, []).append((q, r))
    for key in sorted(classes):
        part = None
        for q, r in classes[key]:
            rest = math.sqrt(p * p + q * q + r * r)
            nb = [e_ref[r + W, c, x + (W + p), W + q : W + q + depth] for c in range(3)]
            bx = nb[0] - center_x
            bz = nb[1] - center_z[q]
            by = nb[2] - center[2]
            square = bx * bx + bz * bz + by * by
            h = jnp.float32(1.0 / rest) - lax.rsqrt(square)
            g = mask_ref[INDEX[p, q, r], x] * h
            force[0] = force[0] + g * bx
            force[1] = force[1] + g * bz
            force[2] = force[2] + g * by
            if energy is not None:
                e = g * (h * square)
                part = e if part is None else part + e
        if energy is not None:
            energy = energy + part * jnp.float32(0.25 * rest)
    for c in range(3):
        acc_ref[c, x] = force[c]
    return energy


def step_kernel(
    counts, depth_total, area,
    disp_hbm, vel_hbm, body_hbm, broken_hbm,
    new_disp_ref, new_vel_ref, new_acc_ref, energy_ref,
    disp_ref, vel_ref, body_ref, broken_ref, acc_ref,
    e1_ref, e2_ref, mask_ref, outside_ref,
    slab_ref, pack_ref, own_z, own_0, far_z, far_0, far_x,
    slot_x, slot_y, slot_z, etile_ref,
    in_sem, recv_sem, send_sem, esend_sem, erecv_sem,
):
    nx, ny, nz = counts
    _, rows, depth, width = disp_ref.shape
    ix, iy, iz = (lax.axis_index(axis) for axis in AXES)
    has_z = {-1: iz > 0, 1: iz < nz - 1}
    group_rows = {
        HIGH: list(range(rows - W, rows)) + list(range(W, rows - W)),
        LOW: list(range(W)),
    }
    slab_rows = {g: align(9 * len(group_rows[g])) for g in (HIGH, LOW)}
    far_rows = align(9 * W)
    toward = {HIGH: 1, LOW: -1}

    def device(dx, dy, dz):
        where = {}
        if dx:
            where["gx"] = lax.rem(ix + (dx + nx), nx)
        if dy:
            where["gy"] = lax.rem(iy + (dy + ny), ny)
        if dz:
            where["gz"] = iz + dz
        return where

    inputs = [
        pltpu.make_async_copy(src, dst, in_sem.at[i])
        for i, (src, dst) in enumerate(
            ((disp_hbm, disp_ref), (broken_hbm, broken_ref), (vel_hbm, vel_ref), (body_hbm, body_ref))
        )
    ]
    for copy in inputs:
        copy.start()

    for s, dz in enumerate(SIDES):

        @pl.when(jnp.logical_not(has_z[dz]))
        def _(s=s):
            for ex in range(2):
                for g in (HIGH, LOW):
                    own_z[ex, g, s] = jnp.zeros(own_z.shape[3:], jnp.float32)
                    far_z[ex, g, s] = jnp.zeros(far_z.shape[3:], jnp.float32)

    barrier = pltpu.get_barrier_semaphore()
    dxs = (0, 1) if nx == 2 else (-1, 0, 1)
    sure = 0
    maybe = {-1: 0, 1: 0}
    for dz in (-1, 0, 1):
        for dx in dxs:
            for dy in (-1, 0, 1):
                if (dx, dy, dz) == (0, 0, 0):
                    continue

                def greet(dx=dx, dy=dy, dz=dz):
                    pl.semaphore_signal(
                        barrier, inc=1, device_id=device(dx, dy, dz), device_id_type=MESH
                    )

                if dz == 0:
                    greet()
                    sure += 1
                else:
                    pl.when(has_z[dz])(greet)
                    maybe[dz] += 1
    for axis, count, me in zip(AXES, counts, (ix, iy, iz)):
        for d in range(1, count):
            pl.semaphore_signal(
                barrier, inc=1, device_id={axis: lax.rem(me + d, count)}, device_id_type=MESH
            )
            sure += 1

    lane = lax.broadcasted_iota(jnp.int32, (depth, width), 1)

    def stage(ex, g, src):
        pack = jnp.zeros((depth, width), jnp.float32)
        for k, x in enumerate(group_rows[g]):
            for c in range(3):
                tile = src[c, x]
                at = 9 * k + 3 * c
                slab_ref[ex, g, 0, at : at + W] = tile[:W]
                slab_ref[ex, g, 1, at : at + W] = tile[depth - W :]
                at = 6 * (3 * k + c)
                moved = pltpu.roll(tile, W + at, 1)
                pack = jnp.where((lane >= at) & (lane < at + 2 * W), moved, pack)
        pack_ref[ex, g] = pack

    def copies(ex, g, src):
        out = []

        def add(src_ref, dst_ref, kind, dx, dy, dz):
            out.append(
                (
                    dz,
                    pltpu.make_async_remote_copy(
                        src_ref=src_ref,
                        dst_ref=dst_ref,
                        send_sem=send_sem.at[ex, g, len(out)],
                        recv_sem=recv_sem.at[ex, g, kind],
                        device_id=device(dx, dy, dz),
                        device_id_type=MESH,
                    ),
                )
            )

        n = slab_rows[g]
        t = toward[g]
        for s, dz in enumerate(SIDES):
            add(slab_ref.at[ex, g, s, 0:n], own_z.at[ex, g, 1 - s, 0:n], 1 - s, 0, 0, dz)
        for i, dy in enumerate(SIDES):
            edge = pl.ds(8 * (1 - i), 8)
            add(pack_ref.at[ex, g], own_0.at[ex, g, edge], 2, 0, dy, 0)
            for s, dz in enumerate(SIDES):
                edge = pl.ds(n + 8 * (1 - i), 8)
                add(pack_ref.at[ex, g], own_z.at[ex, g, 1 - s, edge], 1 - s, 0, dy, dz)
        first = rows - W if g == HIGH else 0
        add(src.at[:, first : first + W], far_x.at[ex, g], 6, t, 0, 0)
        for s, dz in enumerate(SIDES):
            add(
                slab_ref.at[ex, g, s, 0:far_rows], far_z.at[ex, g, 1 - s, 0:far_rows],
                3 + 1 - s, t, 0, dz,
            )
        for i, dy in enumerate(SIDES):
            edge = pl.ds(8 * (1 - i), 8)
            add(pack_ref.at[ex, g], far_0.at[ex, g, edge], 5, t, dy, 0)
            for s, dz in enumerate(SIDES):
                edge = pl.ds(far_rows + 8 * (1 - i), 8)
                add(pack_ref.at[ex, g], far_z.at[ex, g, 1 - s, edge], 3 + 1 - s, t, dy, dz)
        return out

    def each(pairs, act):
        for want in (0, -1, 1):

            def run(want=want):
                for dz, copy in pairs:
                    if dz == want:
                        act(copy)

            if want == 0:
                run()
            else:
                pl.when(has_z[want])(run)

    def arrived(ref, ex, g, kind):
        pltpu.make_async_copy(ref, ref, recv_sem.at[ex, g, kind]).wait()

    def wait_own(ex, g):
        arrived(own_0.at[ex, g], ex, g, 2)
        for s, dz in enumerate(SIDES):
            pl.when(has_z[dz])(
                functools.partial(
                    arrived, own_z.at[ex, g, s, 0 : slab_rows[g] + 16], ex, g, s
                )
            )

    def wait_far(ex, g):
        arrived(far_0.at[ex, g], ex, g, 5)
        arrived(far_x.at[ex, g], ex, g, 6)
        for s, dz in enumerate(SIDES):
            pl.when(has_z[dz])(
                functools.partial(arrived, far_z.at[ex, g, s, 0 : far_rows + 16], ex, g, 3 + s)
            )

    padded = e1_ref.shape[3]
    wide = lax.broadcasted_iota(jnp.int32, (padded, width), 1)

    def fill(e_ref, ex, g, k, row, far, src):
        z_ref, zero_ref = (far_z, far_0) if far else (own_z, own_0)
        n = far_rows if far else slab_rows[g]
        edges = []
        for i in range(2):
            below = z_ref[ex, g, 0, n + 8 * i : n + 8 * i + 8]
            here = zero_ref[ex, g, 8 * i : 8 * i + 8]
            above = z_ref[ex, g, 1, n + 8 * i : n + 8 * i + 8]
            spare = jnp.zeros((padded - depth - 2 * W, width), jnp.float32)
            edges.append(
                jnp.concatenate([below[depth - W :], here, above[:W], spare], axis=0)
            )
        for c in range(3):
            at = 9 * k + 3 * c
            tile = jnp.concatenate(
                [
                    z_ref[ex, g, 0, at : at + W],
                    src(c),
                    z_ref[ex, g, 1, at : at + W],
                    jnp.zeros((padded - depth - 2 * W, width), jnp.float32),
                ],
                axis=0,
            )
            at = 6 * (3 * k + c)
            side = jnp.where(
                wide < W,
                pltpu.roll(edges[1], (2 * width - at - W) % width, 1),
                pltpu.roll(edges[0], (2 * width - W - at) % width, 1),
            )
            for r in REACH:
                if r == 0:
                    moved = tile
                elif r > 0:
                    moved = pltpu.roll(jnp.where(wide < r, side, tile), width - r, 1)
                else:
                    moved = pltpu.roll(jnp.where(wide >= width + r, side, tile), -r, 1)
                if c == 2 and r != 0:
                    moved = moved + float(r)
                e_ref[r + W, c, row] = moved

    def fill_own(e_ref, ex, g, src):
        for k, x in enumerate(group_rows[g]):
            fill(e_ref, ex, g, k, x + W, False, lambda c, x=x: src[c, x])

    def fill_far(e_ref, ex, g):
        for k in range(W):
            row = k if g == HIGH else rows + W + k
            fill(e_ref, ex, g, k, row, True, lambda c, k=k: far_x[ex, g, c, k])

    inputs[0].wait()
    for g in (HIGH, LOW):
        stage(0, g, disp_ref)

    expected = sure
    for dz in SIDES:
        expected = expected + jnp.where(has_z[dz], maybe[dz], 0)
    pl.semaphore_wait(barrier, expected)

    for g in (HIGH, LOW):
        each(copies(0, g, disp_ref), lambda copy: copy.start())

    inputs[1].wait()
    store_masks(broken_ref, mask_ref, outside_ref, iz * depth, depth_total)
    inputs[2].wait()
    inputs[3].wait()
    acc_ref[...] = body_ref[...]
    new_acc_ref[...] = body_ref[...]
    etile_ref[...] = jnp.zeros_like(etile_ref)

    for g in (HIGH, LOW):
        wait_own(0, g)
    for g in (HIGH, LOW):
        fill_own(e1_ref, 0, g, disp_ref)

    def first(i, carry):
        @pl.when(i == rows - 2 * W)
        def _():
            for g in (HIGH, LOW):
                wait_far(0, g)
            for g in (HIGH, LOW):
                fill_far(e1_ref, 0, g)

        x = lax.rem(i + W, rows)
        for p in REACH:
            row_bonds(p, x, e1_ref, mask_ref, acc_ref, depth, None)
        for c in range(3):
            a = acc_ref[c, x]
            v = vel_ref[c, x]
            new_disp_ref[c, x] = (
                disp_ref[c, x] + TIME_STEP * v + 0.5 * TIME_STEP * TIME_STEP * a
            )
            new_vel_ref[c, x] = v + 0.5 * TIME_STEP * a

        @pl.when(i == rows - W - 1)
        def _():
            stage(1, HIGH, new_disp_ref)
            each(copies(1, HIGH, new_disp_ref), lambda copy: copy.start())

        return carry

    lax.fori_loop(0, rows, first, 0)
    stage(1, LOW, new_disp_ref)
    each(copies(1, LOW, new_disp_ref), lambda copy: copy.start())

    def second(j, carry):
        @pl.when(j == 0)
        def _():
            wait_own(1, HIGH)
            fill_own(e2_ref, 1, HIGH, new_disp_ref)
            for c in range(3):
                for x in range(W):
                    e2_ref[W, c, x + W, W : W + depth] = new_disp_ref[c, x]

        @pl.when(j == rows - 2 * W)
        def _():
            wait_far(1, HIGH)
            fill_far(e2_ref, 1, HIGH)

        @pl.when(j == rows - W)
        def _():
            wait_own(1, LOW)
            fill_own(e2_ref, 1, LOW, new_disp_ref)
            wait_far(1, LOW)
            fill_far(e2_ref, 1, LOW)

        energy = jnp.zeros(etile_ref.shape, jnp.float32)
        for p in REACH:
            x = lax.rem(j + (W - p + rows), rows)
            energy = row_bonds(p, x, e2_ref, mask_ref, new_acc_ref, depth, energy)
        etile_ref[...] += energy
        return carry

    lax.fori_loop(0, rows, second, 0)
    for c in range(3):
        for x in range(rows):
            new_vel_ref[c, x] = new_vel_ref[c, x] + 0.5 * TIME_STEP * new_acc_ref[c, x]

    at = 0
    value = etile_ref[...]
    for slot, axis, count, me in zip((slot_x, slot_y, slot_z), AXES, counts, (ix, iy, iz)):
        slot[me] = value
        moves = []
        for d in range(1, count):
            copy = pltpu.make_async_remote_copy(
                src_ref=slot.at[me],
                dst_ref=slot.at[me],
                send_sem=esend_sem.at[at],
                recv_sem=erecv_sem.at[at],
                device_id={axis: lax.rem(me + d, count)},
                device_id_type=MESH,
            )
            copy.start()
            moves.append(copy)
            at += 1
        for copy in moves:
            copy.wait()
        value = slot[0]
        for i in range(1, count):
            value = value + slot[i]
    energy_ref[0, 0] = jnp.sum(value) * jnp.float32(1.0 / area)

    for ex, src in ((0, disp_ref), (1, new_disp_ref)):
        for g in (HIGH, LOW):
            each(copies(ex, g, src), lambda copy: copy.wait_send())


def per_device(displacement, velocity, body_force, broken):
    counts = tuple(lax.axis_size(axis) for axis in AXES)
    _, rows, depth, width = displacement.shape
    area = rows * counts[0] * width * counts[1]
    padded = align(depth + 2 * W)
    slab = align(9 * (rows - W))
    far = align(9 * W)
    peers = sum(counts) - len(counts)
    block = pltpu.VMEM((3, rows, depth, width), jnp.float32)
    out = jax.ShapeDtypeStruct((3, rows, depth, width), jnp.float32)
    vmem = pl.BlockSpec(memory_space=pltpu.VMEM)
    e_shape = pltpu.VMEM((2 * W + 1, 3, rows + 2 * W, padded, width), jnp.float32)
    new_disp, new_vel, new_acc, energy = pl.pallas_call(
        functools.partial(step_kernel, counts, depth * counts[2], area),
        out_shape=(out, out, out, jax.ShapeDtypeStruct((1, 1), jnp.float32)),
        in_specs=[pl.BlockSpec(memory_space=pl.ANY)] * 4,
        out_specs=(vmem, vmem, vmem, pl.BlockSpec(memory_space=pltpu.SMEM)),
        scratch_shapes=[
            block, block, block,
            pltpu.VMEM((broken.shape[0], rows, depth, width), jnp.int32),
            block,
            e_shape, e_shape,
            pltpu.VMEM((len(BONDS), rows, depth, width), jnp.float32),
            pltpu.VMEM((WORD_COUNT, depth, width), jnp.int32),
            pltpu.VMEM((2, 2, 2, slab, width), jnp.float32),
            pltpu.VMEM((2, 2, depth, width), jnp.float32),
            pltpu.VMEM((2, 2, 2, slab + 16, width), jnp.float32),
            pltpu.VMEM((2, 2, 16, width), jnp.float32),
            pltpu.VMEM((2, 2, 2, far + 16, width), jnp.float32),
            pltpu.VMEM((2, 2, 16, width), jnp.float32),
            pltpu.VMEM((2, 2, 3, W, depth, width), jnp.float32),
        ]
        + [pltpu.VMEM((count, depth, width), jnp.float32) for count in counts]
        + [
            pltpu.VMEM((depth, width), jnp.float32),
            pltpu.SemaphoreType.DMA((4,)),
            pltpu.SemaphoreType.DMA((2, 2, 7)),
            pltpu.SemaphoreType.DMA((2, 2, 17)),
            pltpu.SemaphoreType.DMA((peers,)),
            pltpu.SemaphoreType.DMA((peers,)),
        ],
        compiler_params=pltpu.CompilerParams(
            collective_id=0, has_side_effects=True, vmem_limit_bytes=48 * 1024 * 1024
        ),
    )(displacement, velocity, body_force, broken)
    return new_disp, new_vel, new_acc, energy.reshape(())


def solution(mesh):
    spec = P(None, "gx", "gz", "gy")
    return jax.shard_map(
        per_device,
        mesh=mesh,
        in_specs=(spec,) * 4,
        out_specs=(spec, spec, spec, P()),
        check_vma=False,
    )
```

```python
import functools
import math

import jax
import jax.numpy as jnp
from jax import lax
from jax.experimental import pallas as pl
from jax.experimental.pallas import tpu as pltpu
from jax.sharding import PartitionSpec as P

TIME_STEP = 0.05
MICRO_MODULUS = 4.0
BITS_PER_WORD = 30
W = 3
REACH = range(-W, W + 1)
BONDS = tuple(
    (p, q, r) for p in REACH for q in REACH for r in REACH if (p, q, r) != (0, 0, 0)
)
INDEX = {bond: k for k, bond in enumerate(BONDS)}
WORD_COUNT = -(-len(BONDS) // BITS_PER_WORD)
AXES = ("gx", "gy", "gz")
MESH = pl.DeviceIdType.MESH
HIGH, LOW = 0, 1
SIDES = (-1, 1)


def align(n):
    return -(-n // 8) * 8


def depth_bits(shape, depth_start, depth_total):
    depth = lax.broadcasted_iota(jnp.int32, shape, 0) + depth_start
    words = [jnp.zeros(shape, jnp.int32) for _ in range(WORD_COUNT)]
    for q in REACH:
        if q == 0:
            continue
        outside = (depth + q < 0) | (depth + q >= depth_total)
        for w in range(WORD_COUNT):
            bits = 0
            for (p, q2, r), k in INDEX.items():
                if q2 == q and k // BITS_PER_WORD == w:
                    bits |= 1 << (k % BITS_PER_WORD)
            if bits:
                words[w] = words[w] | jnp.where(outside, bits, 0)
    return words


def store_masks(broken_ref, mask_ref, outside_ref, depth_start, depth_total):
    rows = broken_ref.shape[1]
    for w, word in enumerate(depth_bits(broken_ref.shape[2:], depth_start, depth_total)):
        outside_ref[w] = word

    def body(x, carry):
        for w in range(WORD_COUNT):
            word = broken_ref[w, x] | outside_ref[w]
            for k in range(w * BITS_PER_WORD, min(len(BONDS), (w + 1) * BITS_PER_WORD)):
                p, q, r = BONDS[k]
                weight = MICRO_MODULUS * math.exp(-(p * p + q * q + r * r) / 9.0)
                bit = word & (1 << (k % BITS_PER_WORD))
                mask_ref[k, x] = jnp.where(bit == 0, jnp.float32(weight), jnp.float32(0.0))
        return carry

    lax.fori_loop(0, rows, body, 0)


def row_bonds(p, x, e_ref, mask_ref, acc_ref, depth, energy):
    center = [e_ref[W, c, x + W, W : W + depth] for c in range(3)]
    force = [acc_ref[c, x] for c in range(3)]
    center_x = center[0] - float(p)
    center_z = {q: center[1] - float(q) for q in REACH}
    classes = {}
    for q in REACH:
        for r in REACH:
            if (p, q, r) != (0, 0, 0):
                key = 0 if energy is None else q * q + r * r
                classes.setdefault(key, []).append((q, r))
    for key in sorted(classes):
        part = None
        for q, r in classes[key]:
            rest = math.sqrt(p * p + q * q + r * r)
            nb = [e_ref[r + W, c, x + (W + p), W + q : W + q + depth] for c in range(3)]
            bx = nb[0] - center_x
            bz = nb[1] - center_z[q]
            by = nb[2] - center[2]
            square = bx * bx + bz * bz + by * by
            h = jnp.float32(1.0 / rest) - lax.rsqrt(square)
            g = mask_ref[INDEX[p, q, r], x] * h
            force[0] = force[0] + g * bx
            force[1] = force[1] + g * bz
            force[2] = force[2] + g * by
            if energy is not None:
                e = g * (h * square)
                part = e if part is None else part + e
        if energy is not None:
            energy = energy + part * jnp.float32(0.25 * rest)
    for c in range(3):
        acc_ref[c, x] = force[c]
    return energy


def step_kernel(
    counts, depth_total, area, direct,
    disp_hbm, vel_hbm, body_hbm, broken_hbm,
    acc_ref, force_ref, energy_ref,
    disp_ref, vel_ref, body_ref, broken_ref, new_disp_ref,
    e1_ref, e2_ref, mask_ref, outside_ref,
    slab_ref, pack_ref, own_z, own_0, far_z, far_0, far_x,
    slots, etile_ref,
    in_sem, recv_sem, send_sem, esend_sem, erecv_sem,
):
    nx, ny, nz = counts
    _, rows, depth, width = disp_ref.shape
    ix, iy, iz = (lax.axis_index(axis) for axis in AXES)
    has_z = {-1: iz > 0, 1: iz < nz - 1}
    group_rows = {
        HIGH: list(range(rows - W, rows)) + list(range(W, rows - W)),
        LOW: list(range(W)),
    }
    slab_rows = {g: align(9 * len(group_rows[g])) for g in (HIGH, LOW)}
    far_rows = align(9 * W)
    toward = {HIGH: 1, LOW: -1}

    def device(dx, dy, dz):
        where = {}
        if dx:
            where["gx"] = lax.rem(ix + (dx + nx), nx)
        if dy:
            where["gy"] = lax.rem(iy + (dy + ny), ny)
        if dz:
            where["gz"] = iz + dz
        return where

    inputs = [
        pltpu.make_async_copy(src, dst, in_sem.at[i])
        for i, (src, dst) in enumerate(
            ((disp_hbm, disp_ref), (broken_hbm, broken_ref), (vel_hbm, vel_ref), (body_hbm, body_ref))
        )
    ]
    for copy in inputs:
        copy.start()

    for s, dz in enumerate(SIDES):

        @pl.when(jnp.logical_not(has_z[dz]))
        def _(s=s):
            for ex in range(2):
                for g in (HIGH, LOW):
                    own_z[ex, g, s] = jnp.zeros(own_z.shape[3:], jnp.float32)
                    far_z[ex, g, s] = jnp.zeros(far_z.shape[3:], jnp.float32)

    barrier = pltpu.get_barrier_semaphore()
    dxs = (0, 1) if nx == 2 else (-1, 0, 1)
    sure = 0
    maybe = {-1: 0, 1: 0}
    for dz in (-1, 0, 1):
        for dx in dxs:
            for dy in (-1, 0, 1):
                if (dx, dy, dz) == (0, 0, 0):
                    continue

                def greet(dx=dx, dy=dy, dz=dz):
                    pl.semaphore_signal(
                        barrier, inc=1, device_id=device(dx, dy, dz), device_id_type=MESH
                    )

                if dz == 0:
                    greet()
                    sure += 1
                else:
                    pl.when(has_z[dz])(greet)
                    maybe[dz] += 1
    for axis, count, me in zip(AXES, counts, (ix, iy, iz)) if not direct else ():
        for d in range(1, count):
            pl.semaphore_signal(
                barrier, inc=1, device_id={axis: lax.rem(me + d, count)}, device_id_type=MESH
            )
            sure += 1

    lane = lax.broadcasted_iota(jnp.int32, (depth, width), 1)

    def stage(ex, g, src):
        pack = jnp.zeros((depth, width), jnp.float32)
        for k, x in enumerate(group_rows[g]):
            for c in range(3):
                tile = src[c, x]
                at = 9 * k + 3 * c
                slab_ref[ex, g, 0, at : at + W] = tile[:W]
                slab_ref[ex, g, 1, at : at + W] = tile[depth - W :]
                at = 6 * (3 * k + c)
                moved = pltpu.roll(tile, W + at, 1)
                pack = jnp.where((lane >= at) & (lane < at + 2 * W), moved, pack)
        pack_ref[ex, g] = pack

    def copies(ex, g, src):
        out = []

        def add(src_ref, dst_ref, kind, dx, dy, dz):
            out.append(
                (
                    dz,
                    pltpu.make_async_remote_copy(
                        src_ref=src_ref,
                        dst_ref=dst_ref,
                        send_sem=send_sem.at[ex, g, len(out)],
                        recv_sem=recv_sem.at[ex, g, kind],
                        device_id=device(dx, dy, dz),
                        device_id_type=MESH,
                    ),
                )
            )

        n = slab_rows[g]
        t = toward[g]
        for s, dz in enumerate(SIDES):
            add(slab_ref.at[ex, g, s, 0:n], own_z.at[ex, g, 1 - s, 0:n], 1 - s, 0, 0, dz)
        for i, dy in enumerate(SIDES):
            edge = pl.ds(8 * (1 - i), 8)
            add(pack_ref.at[ex, g], own_0.at[ex, g, edge], 2, 0, dy, 0)
            for s, dz in enumerate(SIDES):
                edge = pl.ds(n + 8 * (1 - i), 8)
                add(pack_ref.at[ex, g], own_z.at[ex, g, 1 - s, edge], 1 - s, 0, dy, dz)
        first = rows - W if g == HIGH else 0
        add(src.at[:, first : first + W], far_x.at[ex, g], 6, t, 0, 0)
        for s, dz in enumerate(SIDES):
            add(
                slab_ref.at[ex, g, s, 0:far_rows], far_z.at[ex, g, 1 - s, 0:far_rows],
                3 + 1 - s, t, 0, dz,
            )
        for i, dy in enumerate(SIDES):
            edge = pl.ds(8 * (1 - i), 8)
            add(pack_ref.at[ex, g], far_0.at[ex, g, edge], 5, t, dy, 0)
            for s, dz in enumerate(SIDES):
                edge = pl.ds(far_rows + 8 * (1 - i), 8)
                add(pack_ref.at[ex, g], far_z.at[ex, g, 1 - s, edge], 3 + 1 - s, t, dy, dz)
        return out

    def each(pairs, act):
        for want in (0, -1, 1):

            def run(want=want):
                for dz, copy in pairs:
                    if dz == want:
                        act(copy)

            if want == 0:
                run()
            else:
                pl.when(has_z[want])(run)

    def arrived(ref, ex, g, kind):
        pltpu.make_async_copy(ref, ref, recv_sem.at[ex, g, kind]).wait()

    def wait_own(ex, g):
        arrived(own_0.at[ex, g], ex, g, 2)
        for s, dz in enumerate(SIDES):
            pl.when(has_z[dz])(
                functools.partial(
                    arrived, own_z.at[ex, g, s, 0 : slab_rows[g] + 16], ex, g, s
                )
            )

    def wait_far(ex, g):
        arrived(far_0.at[ex, g], ex, g, 5)
        arrived(far_x.at[ex, g], ex, g, 6)
        for s, dz in enumerate(SIDES):
            pl.when(has_z[dz])(
                functools.partial(arrived, far_z.at[ex, g, s, 0 : far_rows + 16], ex, g, 3 + s)
            )

    padded = e1_ref.shape[3]
    wide = lax.broadcasted_iota(jnp.int32, (padded, width), 1)

    def fill(e_ref, ex, g, k, row, far, src):
        z_ref, zero_ref = (far_z, far_0) if far else (own_z, own_0)
        n = far_rows if far else slab_rows[g]
        edges = []
        for i in range(2):
            below = z_ref[ex, g, 0, n + 8 * i : n + 8 * i + 8]
            here = zero_ref[ex, g, 8 * i : 8 * i + 8]
            above = z_ref[ex, g, 1, n + 8 * i : n + 8 * i + 8]
            spare = jnp.zeros((padded - depth - 2 * W, width), jnp.float32)
            edges.append(
                jnp.concatenate([below[depth - W :], here, above[:W], spare], axis=0)
            )
        for c in range(3):
            at = 9 * k + 3 * c
            tile = jnp.concatenate(
                [
                    z_ref[ex, g, 0, at : at + W],
                    src(c),
                    z_ref[ex, g, 1, at : at + W],
                    jnp.zeros((padded - depth - 2 * W, width), jnp.float32),
                ],
                axis=0,
            )
            at = 6 * (3 * k + c)
            side = jnp.where(
                wide < W,
                pltpu.roll(edges[1], (2 * width - at - W) % width, 1),
                pltpu.roll(edges[0], (2 * width - W - at) % width, 1),
            )
            for r in REACH:
                if r == 0:
                    moved = tile
                elif r > 0:
                    moved = pltpu.roll(jnp.where(wide < r, side, tile), width - r, 1)
                else:
                    moved = pltpu.roll(jnp.where(wide >= width + r, side, tile), -r, 1)
                if c == 2 and r != 0:
                    moved = moved + float(r)
                e_ref[r + W, c, row] = moved

    def fill_own(e_ref, ex, g, src):
        for k, x in enumerate(group_rows[g]):
            fill(e_ref, ex, g, k, x + W, False, lambda c, x=x: src[c, x])

    def fill_far(e_ref, ex, g):
        for k in range(W):
            row = k if g == HIGH else rows + W + k
            fill(e_ref, ex, g, k, row, True, lambda c, k=k: far_x[ex, g, c, k])

    inputs[0].wait()
    for g in (HIGH, LOW):
        stage(0, g, disp_ref)

    expected = sure
    for dz in SIDES:
        expected = expected + jnp.where(has_z[dz], maybe[dz], 0)
    pl.semaphore_wait(barrier, expected)

    for g in (HIGH, LOW):
        each(copies(0, g, disp_ref), lambda copy: copy.start())

    inputs[1].wait()
    store_masks(broken_ref, mask_ref, outside_ref, iz * depth, depth_total)
    inputs[2].wait()
    inputs[3].wait()
    acc_ref[...] = body_ref[...]
    force_ref[...] = jnp.zeros_like(force_ref)
    etile_ref[...] = jnp.zeros_like(etile_ref)

    for g in (HIGH, LOW):
        wait_own(0, g)
    for g in (HIGH, LOW):
        fill_own(e1_ref, 0, g, disp_ref)

    def first(i, carry):
        @pl.when(i == rows - 2 * W)
        def _():
            for g in (HIGH, LOW):
                wait_far(0, g)
            for g in (HIGH, LOW):
                fill_far(e1_ref, 0, g)

        x = lax.rem(i + W, rows)
        for p in REACH:
            row_bonds(p, x, e1_ref, mask_ref, acc_ref, depth, None)
        for c in range(3):
            a = acc_ref[c, x]
            v = vel_ref[c, x]
            new_disp_ref[c, x] = (
                disp_ref[c, x] + TIME_STEP * v + 0.5 * TIME_STEP * TIME_STEP * a
            )

        @pl.when(i == rows - W - 1)
        def _():
            stage(1, HIGH, new_disp_ref)
            each(copies(1, HIGH, new_disp_ref), lambda copy: copy.start())

        return carry

    lax.fori_loop(0, rows, first, 0)
    stage(1, LOW, new_disp_ref)
    each(copies(1, LOW, new_disp_ref), lambda copy: copy.start())

    def second(j, carry):
        @pl.when(j == 0)
        def _():
            wait_own(1, HIGH)
            fill_own(e2_ref, 1, HIGH, new_disp_ref)
            for c in range(3):
                for x in range(W):
                    e2_ref[W, c, x + W, W : W + depth] = new_disp_ref[c, x]

        @pl.when(j == rows - 2 * W)
        def _():
            wait_far(1, HIGH)
            fill_far(e2_ref, 1, HIGH)

        @pl.when(j == rows - W)
        def _():
            wait_own(1, LOW)
            fill_own(e2_ref, 1, LOW, new_disp_ref)
            wait_far(1, LOW)
            fill_far(e2_ref, 1, LOW)

        energy = jnp.zeros(etile_ref.shape, jnp.float32)
        for p in REACH:
            x = lax.rem(j + (W - p + rows), rows)
            energy = row_bonds(p, x, e2_ref, mask_ref, force_ref, depth, energy)
        etile_ref[...] += energy
        return carry

    lax.fori_loop(0, rows, second, 0)
    moves = []
    if direct:
        me = (ix * ny + iy) * nz + iz
        slots[me] = jnp.sum(etile_ref[...], axis=0, keepdims=True)
        for d in range(1, nx * ny * nz):
            dx, dy, dz = d // (ny * nz), d // nz % ny, d % nz
            copy = pltpu.make_async_remote_copy(
                src_ref=slots.at[me],
                dst_ref=slots.at[me],
                send_sem=esend_sem.at[d],
                recv_sem=erecv_sem.at[d],
                device_id={
                    "gx": lax.rem(ix + dx, nx),
                    "gy": lax.rem(iy + dy, ny),
                    "gz": lax.rem(iz + dz, nz),
                },
                device_id_type=MESH,
            )
            copy.start()
            moves.append(copy)
        for copy in moves:
            copy.wait()
        value = slots[...]
    else:
        value = jnp.sum(etile_ref[...], axis=0, keepdims=True)
        at = 0
        for axis, count, me in zip(AXES, counts, (ix, iy, iz)):
            base = at + AXES.index(axis)
            slots[base + me] = value
            moves = []
            for d in range(1, count):
                copy = pltpu.make_async_remote_copy(
                    src_ref=slots.at[base + me],
                    dst_ref=slots.at[base + me],
                    send_sem=esend_sem.at[at],
                    recv_sem=erecv_sem.at[at],
                    device_id={axis: lax.rem(me + d, count)},
                    device_id_type=MESH,
                )
                copy.start()
                moves.append(copy)
                at += 1
            for copy in moves:
                copy.wait()
            value = slots[base]
            for i in range(1, count):
                value = value + slots[base + i]
    energy_ref[0, 0] = jnp.sum(value) * jnp.float32(1.0 / area)

    for ex, src in ((0, disp_ref), (1, new_disp_ref)):
        for g in (HIGH, LOW):
            each(copies(ex, g, src), lambda copy: copy.wait_send())


def per_device(displacement, velocity, body_force, broken):
    counts = tuple(lax.axis_size(axis) for axis in AXES)
    _, rows, depth, width = displacement.shape
    area = rows * counts[0] * width * counts[1]
    padded = align(depth + 2 * W)
    slab = align(9 * (rows - W))
    far = align(9 * W)
    devices = math.prod(counts)
    direct = devices if devices <= 64 else 0
    peers = max(direct, sum(counts))
    block = pltpu.VMEM((3, rows, depth, width), jnp.float32)
    out = jax.ShapeDtypeStruct((3, rows, depth, width), jnp.float32)
    vmem = pl.BlockSpec(memory_space=pltpu.VMEM)
    e_shape = pltpu.VMEM((2 * W + 1, 3, rows + 2 * W, padded, width), jnp.float32)
    acc, force, energy = pl.pallas_call(
        functools.partial(step_kernel, counts, depth * counts[2], area, direct),
        out_shape=(out, out, jax.ShapeDtypeStruct((1, 1), jnp.float32)),
        in_specs=[pl.BlockSpec(memory_space=pltpu.HBM)] * 4,
        out_specs=(vmem, vmem, pl.BlockSpec(memory_space=pltpu.SMEM)),
        scratch_shapes=[
            block, block, block,
            pltpu.VMEM((broken.shape[0], rows, depth, width), jnp.int32),
            block,
            e_shape, e_shape,
            pltpu.VMEM((len(BONDS), rows, depth, width), jnp.float32),
            pltpu.VMEM((WORD_COUNT, depth, width), jnp.int32),
            pltpu.VMEM((2, 2, 2, slab, width), jnp.float32),
            pltpu.VMEM((2, 2, depth, width), jnp.float32),
            pltpu.VMEM((2, 2, 2, slab + 16, width), jnp.float32),
            pltpu.VMEM((2, 2, 16, width), jnp.float32),
            pltpu.VMEM((2, 2, 2, far + 16, width), jnp.float32),
            pltpu.VMEM((2, 2, 16, width), jnp.float32),
            pltpu.VMEM((2, 2, 3, W, depth, width), jnp.float32),
        ]
        + [
            pltpu.VMEM((max(direct, sum(counts)), 1, width), jnp.float32),
            pltpu.VMEM((depth, width), jnp.float32),
            pltpu.SemaphoreType.DMA((4,)),
            pltpu.SemaphoreType.DMA((2, 2, 7)),
            pltpu.SemaphoreType.DMA((2, 2, 17)),
            pltpu.SemaphoreType.DMA((peers,)),
            pltpu.SemaphoreType.DMA((peers,)),
        ],
        compiler_params=pltpu.CompilerParams(
            collective_id=0, has_side_effects=True, vmem_limit_bytes=67043328
        ),
    )(displacement, velocity, body_force, broken)
    new_displacement = (
        displacement + TIME_STEP * velocity + 0.5 * TIME_STEP * TIME_STEP * acc
    )
    new_acceleration = force + body_force
    new_velocity = velocity + 0.5 * TIME_STEP * (acc + new_acceleration)
    return new_displacement, new_velocity, new_acceleration, energy.reshape(())


def solution(mesh):
    spec = P(None, "gx", "gz", "gy")
    return jax.shard_map(
        per_device,
        mesh=mesh,
        in_specs=(spec,) * 4,
        out_specs=(spec, spec, spec, P()),
        check_vma=False,
    )
```

```python
import functools
import math

import jax
import jax.numpy as jnp
from jax import lax
from jax.experimental import pallas as pl
from jax.experimental.pallas import tpu as pltpu
from jax.sharding import PartitionSpec as P

TIME_STEP = 0.05
MICRO_MODULUS = 4.0
BITS_PER_WORD = 30
W = 3
REACH = range(-W, W + 1)
BONDS = tuple(
    (p, q, r) for p in REACH for q in REACH for r in REACH if (p, q, r) != (0, 0, 0)
)
INDEX = {bond: k for k, bond in enumerate(BONDS)}
WORD_COUNT = -(-len(BONDS) // BITS_PER_WORD)
AXES = ("gx", "gy", "gz")
MESH = pl.DeviceIdType.MESH
HIGH, LOW = 0, 1
SIDES = (-1, 1)


def align(n):
    return -(-n // 8) * 8


def depth_bits(shape, depth_start, depth_total):
    depth = lax.broadcasted_iota(jnp.int32, shape, 0) + depth_start
    words = [jnp.zeros(shape, jnp.int32) for _ in range(WORD_COUNT)]
    for q in REACH:
        if q == 0:
            continue
        outside = (depth + q < 0) | (depth + q >= depth_total)
        for w in range(WORD_COUNT):
            bits = 0
            for (p, q2, r), k in INDEX.items():
                if q2 == q and k // BITS_PER_WORD == w:
                    bits |= 1 << (k % BITS_PER_WORD)
            if bits:
                words[w] = words[w] | jnp.where(outside, bits, 0)
    return words


def store_masks(broken_ref, mask_ref, outside_ref, depth_start, depth_total):
    rows = broken_ref.shape[1]
    for w, word in enumerate(depth_bits(broken_ref.shape[2:], depth_start, depth_total)):
        outside_ref[w] = word

    def body(x, carry):
        for w in range(WORD_COUNT):
            word = broken_ref[w, x] | outside_ref[w]
            turned = {r: rotated(word, r) for r in REACH}
            for k in range(w * BITS_PER_WORD, min(len(BONDS), (w + 1) * BITS_PER_WORD)):
                p, q, r = BONDS[k]
                weight = MICRO_MODULUS * math.exp(-(p * p + q * q + r * r) / 9.0)
                bit = turned[r] & (1 << (k % BITS_PER_WORD))
                mask_ref[k, x] = jnp.where(bit == 0, jnp.float32(weight), jnp.float32(0.0))
        return carry

    lax.fori_loop(0, rows, body, 0)


def rotated(tile, r):
    width = tile.shape[1]
    return pltpu.roll(tile, r % width, 1) if r else tile


def bond(p, q, r, x, center_x, center, e_ref, mask_ref):
    rest = math.sqrt(p * p + q * q + r * r)
    bx = e_ref[r + W, q + W, 0, x + (W + p)] - center_x
    bz = e_ref[r + W, q + W, 1, x + (W + p)] - center[1]
    by = e_ref[r + W, q + W, 2, x + (W + p)] - center[2]
    square = bx * bx + bz * bz + by * by
    h = jnp.float32(1.0 / rest) - lax.rsqrt(square)
    return (bx, bz, by), square, h, mask_ref[INDEX[p, q, r], x] * h


def line_force(p, r, x, center, force, e_ref, mask_ref):
    center_x = center[0] - float(p)
    for q in REACH:
        if (p, q, r) != (0, 0, 0):
            b, _, _, g = bond(p, q, r, x, center_x, center, e_ref, mask_ref)
            force = [f + g * d for f, d in zip(force, b)]
    return force


def line_energy(p, r, x, center, e_ref, mask_ref, parts):
    center_x = center[0] - float(p)
    for q in REACH:
        if (p, q, r) != (0, 0, 0):
            _, square, h, g = bond(p, q, r, x, center_x, center, e_ref, mask_ref)
            mask_ref[INDEX[p, q, r], x] = g
            e = g * (h * square)
            key = q * q + r * r
            parts[key] = parts[key] + e if key in parts else e


def tree_sum(terms):
    terms = list(terms)
    while len(terms) > 1:
        pairs = [a + b for a, b in zip(terms[::2], terms[1::2])]
        terms = pairs + terms[len(pairs) * 2 :]
    return terms[0]


def kept_force(r, x, center, e_ref, g_ref):
    lines = []
    for p in REACH:
        kept = [q for q in REACH if (p, q, r) != (0, 0, 0)]
        g = [g_ref[INDEX[p, q, r], x] for q in kept]
        count = tree_sum(g)
        line = [
            tree_sum([a * e_ref[r + W, q + W, c, x + (W + p)] for a, q in zip(g, kept)])
            for c in range(3)
        ]
        if p:
            line[0] = line[0] + float(p) * count
        lines.append(line + [count])
    *force, total = (tree_sum(part) for part in zip(*lines))
    return [f - c * total for f, c in zip(force, center)]


def step_kernel(
    counts, depth_total, area, direct,
    disp_hbm, vel_hbm, body_hbm, broken_hbm,
    acc_hbm, force_hbm, energy_ref,
    disp_ref, vel_ref, body_ref, broken_ref, new_disp_ref, acc_ref, force_ref,
    e1_ref, e2_ref, c1_ref, c2_ref, ext_ref, side_ref, edge_ref,
    mask_ref, outside_ref,
    slab_ref, pack_ref, own_z, own_0, far_z, far_0, far_x,
    slots, etile_ref,
    in_sem, recv_sem, send_sem, esend_sem, erecv_sem,
):
    nx, ny, nz = counts
    _, rows, depth, width = disp_ref.shape
    ix, iy, iz = (lax.axis_index(axis) for axis in AXES)
    has_z = {-1: iz > 0, 1: iz < nz - 1}
    group_rows = {
        HIGH: list(range(rows - W, rows)) + list(range(W, rows - W)),
        LOW: list(range(W)),
    }
    slab_rows = {g: align(9 * len(group_rows[g])) for g in (HIGH, LOW)}
    far_rows = align(9 * W)
    toward = {HIGH: 1, LOW: -1}

    def device(dx, dy, dz):
        where = {}
        if dx:
            where["gx"] = lax.rem(ix + (dx + nx), nx)
        if dy:
            where["gy"] = lax.rem(iy + (dy + ny), ny)
        if dz:
            where["gz"] = iz + dz
        return where

    inputs = [
        pltpu.make_async_copy(src, dst, in_sem.at[i])
        for i, (src, dst) in enumerate(
            ((disp_hbm, disp_ref), (broken_hbm, broken_ref), (vel_hbm, vel_ref), (body_hbm, body_ref))
        )
    ]
    for copy in inputs:
        copy.start()

    for s, dz in enumerate(SIDES):

        @pl.when(jnp.logical_not(has_z[dz]))
        def _(s=s):
            for ex in range(2):
                for g in (HIGH, LOW):
                    own_z[ex, g, s] = jnp.zeros(own_z.shape[3:], jnp.float32)
                    far_z[ex, g, s] = jnp.zeros(far_z.shape[3:], jnp.float32)

    barrier = pltpu.get_barrier_semaphore()
    dxs = (0, 1) if nx == 2 else (-1, 0, 1)
    sure = 0
    maybe = {-1: 0, 1: 0}
    for dz in (-1, 0, 1):
        for dx in dxs:
            for dy in (-1, 0, 1):
                if (dx, dy, dz) == (0, 0, 0):
                    continue

                def greet(dx=dx, dy=dy, dz=dz):
                    pl.semaphore_signal(
                        barrier, inc=1, device_id=device(dx, dy, dz), device_id_type=MESH
                    )

                if dz == 0:
                    greet()
                    sure += 1
                else:
                    pl.when(has_z[dz])(greet)
                    maybe[dz] += 1
    for axis, count, me in zip(AXES, counts, (ix, iy, iz)) if not direct else ():
        for d in range(1, count):
            pl.semaphore_signal(
                barrier, inc=1, device_id={axis: lax.rem(me + d, count)}, device_id_type=MESH
            )
            sure += 1

    lane = lax.broadcasted_iota(jnp.int32, (depth, width), 1)

    def stage(ex, g, src):
        pack = jnp.zeros((depth, width), jnp.float32)
        for k, x in enumerate(group_rows[g]):
            for c in range(3):
                tile = src[c, x]
                at = 9 * k + 3 * c
                slab_ref[ex, g, 0, at : at + W] = tile[:W]
                slab_ref[ex, g, 1, at : at + W] = tile[depth - W :]
                at = 6 * (3 * k + c)
                moved = pltpu.roll(tile, W + at, 1)
                pack = jnp.where((lane >= at) & (lane < at + 2 * W), moved, pack)
        pack_ref[ex, g] = pack

    def copies(ex, g, src):
        out = []

        def add(src_ref, dst_ref, kind, dx, dy, dz):
            out.append(
                (
                    dz,
                    pltpu.make_async_remote_copy(
                        src_ref=src_ref,
                        dst_ref=dst_ref,
                        send_sem=send_sem.at[ex, g, len(out)],
                        recv_sem=recv_sem.at[ex, g, kind],
                        device_id=device(dx, dy, dz),
                        device_id_type=MESH,
                    ),
                )
            )

        n = slab_rows[g]
        t = toward[g]
        for s, dz in enumerate(SIDES):
            add(slab_ref.at[ex, g, s, 0:n], own_z.at[ex, g, 1 - s, 0:n], 1 - s, 0, 0, dz)
        for i, dy in enumerate(SIDES):
            edge = pl.ds(8 * (1 - i), 8)
            add(pack_ref.at[ex, g], own_0.at[ex, g, edge], 2, 0, dy, 0)
            for s, dz in enumerate(SIDES):
                edge = pl.ds(n + 8 * (1 - i), 8)
                add(pack_ref.at[ex, g], own_z.at[ex, g, 1 - s, edge], 1 - s, 0, dy, dz)
        first = rows - W if g == HIGH else 0
        add(src.at[:, first : first + W], far_x.at[ex, g], 6, t, 0, 0)
        for s, dz in enumerate(SIDES):
            add(
                slab_ref.at[ex, g, s, 0:far_rows], far_z.at[ex, g, 1 - s, 0:far_rows],
                3 + 1 - s, t, 0, dz,
            )
        for i, dy in enumerate(SIDES):
            edge = pl.ds(8 * (1 - i), 8)
            add(pack_ref.at[ex, g], far_0.at[ex, g, edge], 5, t, dy, 0)
            for s, dz in enumerate(SIDES):
                edge = pl.ds(far_rows + 8 * (1 - i), 8)
                add(pack_ref.at[ex, g], far_z.at[ex, g, 1 - s, edge], 3 + 1 - s, t, dy, dz)
        return out

    def each(pairs, act):
        for want in (0, -1, 1):

            def run(want=want):
                for dz, copy in pairs:
                    if dz == want:
                        act(copy)

            if want == 0:
                run()
            else:
                pl.when(has_z[want])(run)

    def arrived(ref, ex, g, kind):
        pltpu.make_async_copy(ref, ref, recv_sem.at[ex, g, kind]).wait()

    def wait_own(ex, g):
        arrived(own_0.at[ex, g], ex, g, 2)
        for s, dz in enumerate(SIDES):
            pl.when(has_z[dz])(
                functools.partial(
                    arrived, own_z.at[ex, g, s, 0 : slab_rows[g] + 16], ex, g, s
                )
            )

    def wait_far(ex, g):
        arrived(far_0.at[ex, g], ex, g, 5)
        arrived(far_x.at[ex, g], ex, g, 6)
        for s, dz in enumerate(SIDES):
            pl.when(has_z[dz])(
                functools.partial(arrived, far_z.at[ex, g, s, 0 : far_rows + 16], ex, g, 3 + s)
            )

    below_w = lane < 0
    for t in range(width // (2 * W)):
        below_w = below_w | ((lane >= 2 * W * t) & (lane < 2 * W * t + W))

    def combine(ex, g, far):
        z_ref, zero_ref = (far_z, far_0) if far else (own_z, own_0)
        n = far_rows if far else slab_rows[g]
        at = 2 * g + far

        def both(ref, *where):
            return jnp.where(
                below_w, ref[(*where, slice(0, 8))], ref[(*where, slice(8, 16))]
            )

        edge_ref[at, 0:W] = both(z_ref.at[ex, g, 0, n : n + 16])[depth - W :]
        edge_ref[at, W : W + depth] = both(zero_ref.at[ex, g])
        edge_ref[at, W + depth : 2 * W + depth] = both(z_ref.at[ex, g, 1, n : n + 16])[:W]
        return edge_ref[at]

    def fill(e_ref, ex, g, k, row, far, edge, src):
        z_ref = far_z if far else own_z
        for c in range(3):
            at = 9 * k + 3 * c
            ext_ref[c, row, 0:W] = z_ref[ex, g, 0, at : at + W]
            ext_ref[c, row, W : W + depth] = src(c)
            ext_ref[c, row, W + depth : 2 * W + depth] = z_ref[ex, g, 1, at : at + W]
            at = 2 * W * (3 * k + c)
            side_ref[c, row] = pltpu.roll(edge, (2 * width - W - at) % width, 1)
            for q in REACH:
                tile = ext_ref[c, row, W + q : W + q + depth]
                side = side_ref[c, row, W + q : W + q + depth]
                if c == 1 and q:
                    tile, side = tile + float(q), side + float(q)
                for r in REACH:
                    if r == 0:
                        value = tile
                    elif r > 0:
                        value = jnp.where(lane < r, side, tile)
                    else:
                        value = jnp.where(lane >= width + r, side, tile)
                    if c == 2 and r:
                        value = value + float(r)
                    e_ref[r + W, q + W, c, row] = value

    def fill_own(e_ref, ex, g, src):
        edge = combine(ex, g, 0)
        for k, x in enumerate(group_rows[g]):
            fill(e_ref, ex, g, k, x + W, 0, edge, lambda c, x=x: src[c, x])

    def fill_far(e_ref, ex, g):
        edge = combine(ex, g, 1)
        for k in range(W):
            row = k if g == HIGH else rows + W + k
            fill(e_ref, ex, g, k, row, 1, edge, lambda c, k=k: far_x[ex, g, c, k])

    def turn(c_ref, x, src):
        for c in range(3):
            for r in REACH:
                c_ref[r + W, c, x] = rotated(src[c, x], r)

    inputs[0].wait()
    for g in (HIGH, LOW):
        stage(0, g, disp_ref)

    expected = sure
    for dz in SIDES:
        expected = expected + jnp.where(has_z[dz], maybe[dz], 0)
    pl.semaphore_wait(barrier, expected)

    for g in (HIGH, LOW):
        each(copies(0, g, disp_ref), lambda copy: copy.start())

    inputs[1].wait()
    store_masks(broken_ref, mask_ref, outside_ref, iz * depth, depth_total)
    inputs[2].wait()
    inputs[3].wait()
    acc_ref[...] = body_ref[...]
    force_ref[...] = jnp.zeros_like(force_ref)
    for x in range(rows):
        turn(c1_ref, x, disp_ref)
    etile_ref[...] = jnp.zeros_like(etile_ref)

    for g in (HIGH, LOW):
        wait_own(0, g)
    for g in (HIGH, LOW):
        fill_own(e1_ref, 0, g, disp_ref)

    def first(i, carry):
        @pl.when(i == rows - 2 * W)
        def _():
            for g in (HIGH, LOW):
                wait_far(0, g)
            for g in (HIGH, LOW):
                fill_far(e1_ref, 0, g)

        x = lax.rem(i + W, rows)
        turn(c2_ref, lax.rem(i + (W - 1), rows), new_disp_ref)
        for r in REACH:
            center = [c1_ref[r + W, c, x] for c in range(3)]
            force = [jnp.zeros((depth, width), jnp.float32)] * 3
            for p in REACH:
                force = line_force(p, r, x, center, force, e1_ref, mask_ref)
            for c in range(3):
                acc_ref[c, x] += rotated(force[c], -r)
        for c in range(3):
            a = acc_ref[c, x]
            v = vel_ref[c, x]
            new_disp_ref[c, x] = (
                disp_ref[c, x] + TIME_STEP * v + 0.5 * TIME_STEP * TIME_STEP * a
            )

        @pl.when(i == rows - W - 1)
        def _():
            stage(1, HIGH, new_disp_ref)
            each(copies(1, HIGH, new_disp_ref), lambda copy: copy.start())

        return carry

    lax.fori_loop(0, rows, first, 0)
    turn(c2_ref, W - 1, new_disp_ref)
    stage(1, LOW, new_disp_ref)
    each(copies(1, LOW, new_disp_ref), lambda copy: copy.start())

    def second(j, carry):
        @pl.when(j == 0)
        def _():
            wait_own(1, HIGH)
            fill_own(e2_ref, 1, HIGH, new_disp_ref)

        @pl.when(j == rows - 2 * W)
        def _():
            wait_far(1, HIGH)
            fill_far(e2_ref, 1, HIGH)

        @pl.when(j == rows - W)
        def _():
            wait_own(1, LOW)
            fill_own(e2_ref, 1, LOW, new_disp_ref)
            wait_far(1, LOW)
            fill_far(e2_ref, 1, LOW)

        energy = jnp.zeros(etile_ref.shape, jnp.float32)
        for p in REACH:
            x = lax.rem(j + (W - p + rows), rows)
            parts = {}
            for r in REACH:
                center = [c2_ref[r + W, c, x] for c in range(3)]
                line_energy(p, r, x, center, e2_ref, mask_ref, parts)
            for key, part in parts.items():
                energy = energy + part * jnp.float32(0.25 * math.sqrt(p * p + key))
        etile_ref[...] += energy
        return carry

    lax.fori_loop(0, rows, second, 0)
    def third(x, carry):
        for r in REACH:
            center = [c2_ref[r + W, c, x] for c in range(3)]
            force = kept_force(r, x, center, e2_ref, mask_ref)
            for c in range(3):
                force_ref[c, x] += rotated(force[c], -r)
        return carry

    results = [
        pltpu.make_async_copy(acc_ref, acc_hbm, in_sem.at[4]),
        pltpu.make_async_copy(force_ref, force_hbm, in_sem.at[5]),
    ]
    results[0].start()

    def sum_force():
        lax.fori_loop(0, rows, third, 0)
        results[1].start()
        for ex, src in ((0, disp_ref), (1, new_disp_ref)):
            for g in (HIGH, LOW):
                each(copies(ex, g, src), lambda copy: copy.wait_send())

    moves = []
    if direct:
        me = (ix * ny + iy) * nz + iz
        slots[me] = jnp.sum(etile_ref[...], axis=0, keepdims=True)
        for d in range(1, nx * ny * nz):
            dx, dy, dz = d // (ny * nz), d // nz % ny, d % nz
            copy = pltpu.make_async_remote_copy(
                src_ref=slots.at[me],
                dst_ref=slots.at[me],
                send_sem=esend_sem.at[d],
                recv_sem=erecv_sem.at[0],
                device_id={
                    "gx": lax.rem(ix + dx, nx),
                    "gy": lax.rem(iy + dy, ny),
                    "gz": lax.rem(iz + dz, nz),
                },
                device_id_type=MESH,
            )
            copy.start()
            moves.append(copy)
        sum_force()
        for copy in moves:
            copy.wait_send()
        landed = slots.at[: nx * ny * nz - 1]
        pltpu.make_async_copy(landed, landed, erecv_sem.at[0]).wait()
        value = slots[...]
    else:
        sum_force()
        value = jnp.sum(etile_ref[...], axis=0, keepdims=True)
        at = 0
        for axis, count, me in zip(AXES, counts, (ix, iy, iz)):
            base = at + AXES.index(axis)
            slots[base + me] = value
            moves = []
            for d in range(1, count):
                copy = pltpu.make_async_remote_copy(
                    src_ref=slots.at[base + me],
                    dst_ref=slots.at[base + me],
                    send_sem=esend_sem.at[at],
                    recv_sem=erecv_sem.at[at],
                    device_id={axis: lax.rem(me + d, count)},
                    device_id_type=MESH,
                )
                copy.start()
                moves.append(copy)
                at += 1
            for copy in moves:
                copy.wait()
            value = slots[base]
            for i in range(1, count):
                value = value + slots[base + i]
    energy_ref[0, 0] = jnp.sum(value) * jnp.float32(1.0 / area)

    for copy in results:
        copy.wait()


def per_device(displacement, velocity, body_force, broken):
    counts = tuple(lax.axis_size(axis) for axis in AXES)
    _, rows, depth, width = displacement.shape
    area = rows * counts[0] * width * counts[1]
    padded = align(depth + 2 * W)
    slab = align(9 * (rows - W))
    far = align(9 * W)
    devices = math.prod(counts)
    direct = devices if devices <= 64 else 0
    peers = max(direct, sum(counts))
    block = pltpu.VMEM((3, rows, depth, width), jnp.float32)
    out = jax.ShapeDtypeStruct((3, rows, depth, width), jnp.float32)
    hbm = pl.BlockSpec(memory_space=pltpu.HBM)
    span = 2 * W + 1
    e_shape = pltpu.VMEM((span, span, 3, rows + 2 * W, depth, width), jnp.float32)
    turned = pltpu.VMEM((span, 3, rows, depth, width), jnp.float32)
    halo = pltpu.VMEM((3, rows + 2 * W, padded, width), jnp.float32)
    acc, force, energy = pl.pallas_call(
        functools.partial(step_kernel, counts, depth * counts[2], area, direct),
        out_shape=(out, out, jax.ShapeDtypeStruct((1, 1), jnp.float32)),
        in_specs=[hbm] * 4,
        out_specs=(hbm, hbm, pl.BlockSpec(memory_space=pltpu.SMEM)),
        scratch_shapes=[
            block, block, block,
            pltpu.VMEM((broken.shape[0], rows, depth, width), jnp.int32),
            block, block, block,
            e_shape, e_shape, turned, turned, halo, halo,
            pltpu.VMEM((4, padded, width), jnp.float32),
            pltpu.VMEM((len(BONDS), rows, depth, width), jnp.float32),
            pltpu.VMEM((WORD_COUNT, depth, width), jnp.int32),
            pltpu.VMEM((2, 2, 2, slab, width), jnp.float32),
            pltpu.VMEM((2, 2, depth, width), jnp.float32),
            pltpu.VMEM((2, 2, 2, slab + 16, width), jnp.float32),
            pltpu.VMEM((2, 2, 16, width), jnp.float32),
            pltpu.VMEM((2, 2, 2, far + 16, width), jnp.float32),
            pltpu.VMEM((2, 2, 16, width), jnp.float32),
            pltpu.VMEM((2, 2, 3, W, depth, width), jnp.float32),
        ]
        + [
            pltpu.VMEM((max(direct, sum(counts)), 1, width), jnp.float32),
            pltpu.VMEM((depth, width), jnp.float32),
            pltpu.SemaphoreType.DMA((6,)),
            pltpu.SemaphoreType.DMA((2, 2, 7)),
            pltpu.SemaphoreType.DMA((2, 2, 17)),
            pltpu.SemaphoreType.DMA((peers,)),
            pltpu.SemaphoreType.DMA((peers,)),
        ],
        compiler_params=pltpu.CompilerParams(
            collective_id=0, has_side_effects=True, vmem_limit_bytes=67043328
        ),
    )(displacement, velocity, body_force, broken)
    new_displacement = (
        displacement + TIME_STEP * velocity + 0.5 * TIME_STEP * TIME_STEP * acc
    )
    new_acceleration = force + body_force
    new_velocity = velocity + 0.5 * TIME_STEP * (acc + new_acceleration)
    return new_displacement, new_velocity, new_acceleration, energy.reshape(())


def solution(mesh):
    spec = P(None, "gx", "gz", "gy")
    return jax.shard_map(
        per_device,
        mesh=mesh,
        in_specs=(spec,) * 4,
        out_specs=(spec, spec, spec, P()),
        check_vma=False,
    )
```

```python
import functools
import math

import jax
import jax.numpy as jnp
from jax import lax
from jax.experimental import pallas as pl
from jax.experimental.pallas import tpu as pltpu
from jax.sharding import PartitionSpec as P

TIME_STEP = 0.05
MICRO_MODULUS = 4.0
BITS_PER_WORD = 30
W = 3
REACH = range(-W, W + 1)
BONDS = tuple(
    (p, q, r) for p in REACH for q in REACH for r in REACH if (p, q, r) != (0, 0, 0)
)
INDEX = {bond: k for k, bond in enumerate(BONDS)}
WORD_COUNT = -(-len(BONDS) // BITS_PER_WORD)
AXES = ("gx", "gy", "gz")
MESH = pl.DeviceIdType.MESH
HIGH, LOW = 0, 1
SIDES = (-1, 1)


def align(n):
    return -(-n // 8) * 8


def depth_bits(shape, depth_start, depth_total):
    depth = lax.broadcasted_iota(jnp.int32, shape, 0) + depth_start
    words = [jnp.zeros(shape, jnp.int32) for _ in range(WORD_COUNT)]
    for q in REACH:
        if q == 0:
            continue
        outside = (depth + q < 0) | (depth + q >= depth_total)
        for w in range(WORD_COUNT):
            bits = 0
            for (p, q2, r), k in INDEX.items():
                if q2 == q and k // BITS_PER_WORD == w:
                    bits |= 1 << (k % BITS_PER_WORD)
            if bits:
                words[w] = words[w] | jnp.where(outside, bits, 0)
    return words


def signed(bits):
    return bits - (1 << 32) if bits >> 31 else bits


def turned_bits(words):
    out = {}
    for r in REACH:
        taken = {}
        for (p, q, r2), k in INDEX.items():
            if r2 == r:
                taken.setdefault(k // BITS_PER_WORD, []).append(k)
        if r == 0:
            for w, ks in taken.items():
                for k in ks:
                    out[k] = (words[w], signed(1 << (k % BITS_PER_WORD)))
            continue
        packs = []
        for w, ks in taken.items():
            at = sum(1 << (k % BITS_PER_WORD) for k in ks)
            shifts = sorted(range(-BITS_PER_WORD, BITS_PER_WORD), key=abs)
            home = None
            for pack in packs:
                for shift in shifts:
                    moved = at << shift if shift >= 0 else at >> -shift
                    whole = (moved >> shift if shift >= 0 else moved << -shift) == at
                    if whole and moved < 1 << 32 and not moved & pack[0]:
                        home = (pack, shift, moved)
                        break
                if home:
                    break
            if home is None:
                packs.append([0, None, []])
                home = (packs[-1], 0, at)
            pack, shift, moved = home
            value = words[w] & at
            if shift > 0:
                value = value << shift
            elif shift < 0:
                value = value >> -shift
            pack[0] |= moved
            pack[1] = value if pack[1] is None else pack[1] | value
            pack[2] += [(k, k % BITS_PER_WORD + shift) for k in ks]
        for _, value, bonds in packs:
            value = rotated(value, r)
            for k, at in bonds:
                out[k] = (value, signed(1 << at))
    return out


def store_masks(broken_ref, mask_ref, outside_ref, depth_start, depth_total):
    rows = broken_ref.shape[1]
    for w, word in enumerate(depth_bits(broken_ref.shape[2:], depth_start, depth_total)):
        outside_ref[w] = word

    def body(x, carry):
        words = [broken_ref[w, x] | outside_ref[w] for w in range(WORD_COUNT)]
        for k, (tile, bit) in turned_bits(words).items():
            p, q, r = BONDS[k]
            weight = MICRO_MODULUS * math.exp(-(p * p + q * q + r * r) / 9.0)
            mask_ref[k, x] = jnp.where(tile & bit == 0, jnp.float32(weight), jnp.float32(0.0))
        return carry

    lax.fori_loop(0, rows, body, 0)


def rotated(tile, r):
    width = tile.shape[1]
    return pltpu.roll(tile, r % width, 1) if r else tile


def bond(p, q, r, x, center_x, center, e_ref, mask_ref):
    rest = math.sqrt(p * p + q * q + r * r)
    bx = e_ref[r + W, q + W, 0, x + (W + p)] - center_x
    bz = e_ref[r + W, q + W, 1, x + (W + p)] - center[1]
    by = e_ref[r + W, q + W, 2, x + (W + p)] - center[2]
    square = bx * bx + bz * bz + by * by
    h = jnp.float32(1.0 / rest) - lax.rsqrt(square)
    return (bx, bz, by), square, h, mask_ref[INDEX[p, q, r], x] * h


def line_force(p, r, x, center, force, e_ref, mask_ref):
    center_x = center[0] - float(p)
    for q in REACH:
        if (p, q, r) != (0, 0, 0):
            b, _, _, g = bond(p, q, r, x, center_x, center, e_ref, mask_ref)
            force = [f + g * d for f, d in zip(force, b)]
    return force


def line_energy(p, r, x, center, e_ref, mask_ref, parts):
    center_x = center[0] - float(p)
    for q in REACH:
        if (p, q, r) != (0, 0, 0):
            _, square, h, g = bond(p, q, r, x, center_x, center, e_ref, mask_ref)
            mask_ref[INDEX[p, q, r], x] = g
            e = g * (h * square)
            key = q * q + r * r
            parts[key] = parts[key] + e if key in parts else e


def tree_sum(terms):
    terms = list(terms)
    while len(terms) > 1:
        pairs = [a + b for a, b in zip(terms[::2], terms[1::2])]
        terms = pairs + terms[len(pairs) * 2 :]
    return terms[0]


def kept_force(r, steps, x, center, e_ref, g_ref):
    lines = []
    for p in steps:
        kept = [q for q in REACH if (p, q, r) != (0, 0, 0)]
        g = [g_ref[INDEX[p, q, r], x] for q in kept]
        count = tree_sum(g)
        line = [
            tree_sum([a * e_ref[r + W, q + W, c, x + (W + p)] for a, q in zip(g, kept)])
            for c in range(3)
        ]
        if p:
            line[0] = line[0] + float(p) * count
        lines.append(line + [count])
    *force, total = (tree_sum(part) for part in zip(*lines))
    return [f - c * total for f, c in zip(force, center)]


def step_kernel(
    counts, depth_total, area, direct,
    disp_hbm, vel_hbm, body_hbm, broken_hbm,
    acc_hbm, force_hbm, energy_ref,
    disp_ref, vel_ref, body_ref, broken_ref, new_disp_ref, acc_ref, force_ref,
    e1_ref, e2_ref, c1_ref, c2_ref, ext_ref, side_ref, edge_ref,
    mask_ref, outside_ref,
    slab_ref, pack_ref, own_z, own_0, far_z, far_0, far_x,
    slots, etile_ref,
    in_sem, recv_sem, send_sem, esend_sem, erecv_sem,
):
    nx, ny, nz = counts
    _, rows, depth, width = disp_ref.shape
    ix, iy, iz = (lax.axis_index(axis) for axis in AXES)
    has_z = {-1: iz > 0, 1: iz < nz - 1}
    group_rows = {
        HIGH: list(range(rows - W, rows)) + list(range(W, rows - W)),
        LOW: list(range(W)),
    }
    slab_rows = {g: align(9 * len(group_rows[g])) for g in (HIGH, LOW)}
    far_rows = align(9 * W)
    toward = {HIGH: 1, LOW: -1}

    def device(dx, dy, dz):
        where = {}
        if dx:
            where["gx"] = lax.rem(ix + (dx + nx), nx)
        if dy:
            where["gy"] = lax.rem(iy + (dy + ny), ny)
        if dz:
            where["gz"] = iz + dz
        return where

    inputs = [
        pltpu.make_async_copy(src, dst, in_sem.at[i])
        for i, (src, dst) in enumerate(
            ((disp_hbm, disp_ref), (broken_hbm, broken_ref), (vel_hbm, vel_ref), (body_hbm, body_ref))
        )
    ]
    for copy in inputs:
        copy.start()

    for s, dz in enumerate(SIDES):

        @pl.when(jnp.logical_not(has_z[dz]))
        def _(s=s):
            for ex in range(2):
                for g in (HIGH, LOW):
                    own_z[ex, g, s] = jnp.zeros(own_z.shape[3:], jnp.float32)
                    far_z[ex, g, s] = jnp.zeros(far_z.shape[3:], jnp.float32)

    barrier = pltpu.get_barrier_semaphore()
    dxs = (0, 1) if nx == 2 else (-1, 0, 1)
    sure = 0
    maybe = {-1: 0, 1: 0}
    for dz in (-1, 0, 1):
        for dx in dxs:
            for dy in (-1, 0, 1):
                if (dx, dy, dz) == (0, 0, 0):
                    continue

                def greet(dx=dx, dy=dy, dz=dz):
                    pl.semaphore_signal(
                        barrier, inc=1, device_id=device(dx, dy, dz), device_id_type=MESH
                    )

                if dz == 0:
                    greet()
                    sure += 1
                else:
                    pl.when(has_z[dz])(greet)
                    maybe[dz] += 1
    for axis, count, me in zip(AXES, counts, (ix, iy, iz)) if not direct else ():
        for d in range(1, count):
            pl.semaphore_signal(
                barrier, inc=1, device_id={axis: lax.rem(me + d, count)}, device_id_type=MESH
            )
            sure += 1

    lane = lax.broadcasted_iota(jnp.int32, (depth, width), 1)

    def stage(ex, g, src):
        pack = jnp.zeros((depth, width), jnp.float32)
        for k, x in enumerate(group_rows[g]):
            for c in range(3):
                tile = src[c, x]
                at = 9 * k + 3 * c
                slab_ref[ex, g, 0, at : at + W] = tile[:W]
                slab_ref[ex, g, 1, at : at + W] = tile[depth - W :]
                at = 6 * (3 * k + c)
                moved = pltpu.roll(tile, W + at, 1)
                pack = jnp.where((lane >= at) & (lane < at + 2 * W), moved, pack)
        pack_ref[ex, g] = pack

    def copies(ex, g, src):
        out = []

        def add(src_ref, dst_ref, kind, dx, dy, dz):
            out.append(
                (
                    dz,
                    pltpu.make_async_remote_copy(
                        src_ref=src_ref,
                        dst_ref=dst_ref,
                        send_sem=send_sem.at[ex, g, dz + 1],
                        recv_sem=recv_sem.at[ex, g, kind],
                        device_id=device(dx, dy, dz),
                        device_id_type=MESH,
                    ),
                )
            )

        n = slab_rows[g]
        t = toward[g]
        for s, dz in enumerate(SIDES):
            add(slab_ref.at[ex, g, s, 0:n], own_z.at[ex, g, 1 - s, 0:n], 1 - s, 0, 0, dz)
        for i, dy in enumerate(SIDES):
            edge = pl.ds(8 * (1 - i), 8)
            add(pack_ref.at[ex, g], own_0.at[ex, g, edge], 2, 0, dy, 0)
            for s, dz in enumerate(SIDES):
                edge = pl.ds(n + 8 * (1 - i), 8)
                add(pack_ref.at[ex, g], own_z.at[ex, g, 1 - s, edge], 1 - s, 0, dy, dz)
        first = rows - W if g == HIGH else 0
        add(src.at[:, first : first + W], far_x.at[ex, g], 6, t, 0, 0)
        for s, dz in enumerate(SIDES):
            add(
                slab_ref.at[ex, g, s, 0:far_rows], far_z.at[ex, g, 1 - s, 0:far_rows],
                3 + 1 - s, t, 0, dz,
            )
        for i, dy in enumerate(SIDES):
            edge = pl.ds(8 * (1 - i), 8)
            add(pack_ref.at[ex, g], far_0.at[ex, g, edge], 5, t, dy, 0)
            for s, dz in enumerate(SIDES):
                edge = pl.ds(far_rows + 8 * (1 - i), 8)
                add(pack_ref.at[ex, g], far_z.at[ex, g, 1 - s, edge], 3 + 1 - s, t, dy, dz)
        return out

    def each(pairs, act):
        for want in (0, -1, 1):

            def run(want=want):
                for dz, copy in pairs:
                    if dz == want:
                        act(copy)

            if want == 0:
                run()
            else:
                pl.when(has_z[want])(run)

    def arrived(ref, ex, g, kind):
        pltpu.make_async_copy(ref, ref, recv_sem.at[ex, g, kind]).wait()

    def wait_sent(ex, g):
        def sent(dz, tiles):
            ref = mask_ref.at[0:tiles, 0]
            pltpu.make_async_copy(ref, ref, send_sem.at[ex, g, dz + 1]).wait()

        sent(0, 4 + 3 * W)
        for dz in SIDES:
            tiles = (slab_rows[g] + far_rows) // 8 + 4
            pl.when(has_z[dz])(functools.partial(sent, dz, tiles))

    def wait_own(ex, g):
        arrived(own_0.at[ex, g], ex, g, 2)
        for s, dz in enumerate(SIDES):
            pl.when(has_z[dz])(
                functools.partial(
                    arrived, own_z.at[ex, g, s, 0 : slab_rows[g] + 16], ex, g, s
                )
            )

    def wait_far(ex, g):
        arrived(far_0.at[ex, g], ex, g, 5)
        arrived(far_x.at[ex, g], ex, g, 6)
        for s, dz in enumerate(SIDES):
            pl.when(has_z[dz])(
                functools.partial(arrived, far_z.at[ex, g, s, 0 : far_rows + 16], ex, g, 3 + s)
            )

    below_w = lane < 0
    for t in range(width // (2 * W)):
        below_w = below_w | ((lane >= 2 * W * t) & (lane < 2 * W * t + W))

    def combine(ex, g, far):
        z_ref, zero_ref = (far_z, far_0) if far else (own_z, own_0)
        n = far_rows if far else slab_rows[g]
        at = 2 * g + far

        def both(ref, *where):
            return jnp.where(
                below_w, ref[(*where, slice(0, 8))], ref[(*where, slice(8, 16))]
            )

        edge_ref[at, 0:W] = both(z_ref.at[ex, g, 0, n : n + 16])[depth - W :]
        edge_ref[at, W : W + depth] = both(zero_ref.at[ex, g])
        edge_ref[at, W + depth : 2 * W + depth] = both(z_ref.at[ex, g, 1, n : n + 16])[:W]
        return edge_ref[at]

    def fill(e_ref, ex, g, k, row, far, edge, src):
        z_ref = far_z if far else own_z
        for c in range(3):
            at = 9 * k + 3 * c
            ext_ref[c, row, 0:W] = z_ref[ex, g, 0, at : at + W]
            ext_ref[c, row, W : W + depth] = src(c)
            ext_ref[c, row, W + depth : 2 * W + depth] = z_ref[ex, g, 1, at : at + W]
            at = 2 * W * (3 * k + c)
            side_ref[c, row] = pltpu.roll(edge, (2 * width - W - at) % width, 1)
            for q in REACH:
                tile = ext_ref[c, row, W + q : W + q + depth]
                side = side_ref[c, row, W + q : W + q + depth]
                if c == 1 and q:
                    tile, side = tile + float(q), side + float(q)
                for r in REACH:
                    if r == 0:
                        value = tile
                    elif r > 0:
                        value = jnp.where(lane < r, side, tile)
                    else:
                        value = jnp.where(lane >= width + r, side, tile)
                    if c == 2 and r:
                        value = value + float(r)
                    e_ref[r + W, q + W, c, row] = value

    def fill_own(e_ref, ex, g, src):
        edge = combine(ex, g, 0)
        for k, x in enumerate(group_rows[g]):
            fill(e_ref, ex, g, k, x + W, 0, edge, lambda c, x=x: src[c, x])

    def fill_far(e_ref, ex, g):
        edge = combine(ex, g, 1)
        for k in range(W):
            row = k if g == HIGH else rows + W + k
            fill(e_ref, ex, g, k, row, 1, edge, lambda c, k=k: far_x[ex, g, c, k])

    def turn(c_ref, x, src):
        for c in range(3):
            for r in REACH:
                c_ref[r + W, c, x] = rotated(src[c, x], r)

    inputs[0].wait()
    for g in (HIGH, LOW):
        stage(0, g, disp_ref)

    expected = sure
    for dz in SIDES:
        expected = expected + jnp.where(has_z[dz], maybe[dz], 0)
    pl.semaphore_wait(barrier, expected)

    pairs = {g: copies(0, g, disp_ref) for g in (HIGH, LOW)}
    for part in (slice(0, 8), slice(8, None)):
        for g in (HIGH, LOW):
            each(pairs[g][part], lambda copy: copy.start())

    inputs[1].wait()
    store_masks(broken_ref, mask_ref, outside_ref, iz * depth, depth_total)
    inputs[2].wait()
    inputs[3].wait()
    acc_ref[...] = body_ref[...]
    force_ref[...] = jnp.zeros_like(force_ref)
    for x in range(rows):
        turn(c1_ref, x, disp_ref)
    etile_ref[...] = jnp.zeros_like(etile_ref)

    for g in (HIGH, LOW):
        wait_own(0, g)
    for g in (HIGH, LOW):
        fill_own(e1_ref, 0, g, disp_ref)

    def first(i, carry):
        @pl.when(i == rows - 2 * W)
        def _():
            for g in (HIGH, LOW):
                wait_far(0, g)
            for g in (HIGH, LOW):
                fill_far(e1_ref, 0, g)

        x = lax.rem(i + W, rows)
        turn(c2_ref, lax.rem(i + (W - 1), rows), new_disp_ref)
        for r in REACH:
            center = [c1_ref[r + W, c, x] for c in range(3)]
            for steps in (REACH[:W], REACH[W:]):
                force = [jnp.zeros((depth, width), jnp.float32)] * 3
                for p in steps:
                    force = line_force(p, r, x, center, force, e1_ref, mask_ref)
                for c in range(3):
                    acc_ref[c, x] += rotated(force[c], -r)
        for c in range(3):
            a = acc_ref[c, x]
            v = vel_ref[c, x]
            new_disp_ref[c, x] = (
                disp_ref[c, x] + TIME_STEP * v + 0.5 * TIME_STEP * TIME_STEP * a
            )

        @pl.when(i == rows - W - 1)
        def _():
            stage(1, HIGH, new_disp_ref)
            each(copies(1, HIGH, new_disp_ref), lambda copy: copy.start())

        return carry

    lax.fori_loop(0, rows, first, 0)
    turn(c2_ref, W - 1, new_disp_ref)
    stage(1, LOW, new_disp_ref)
    each(copies(1, LOW, new_disp_ref), lambda copy: copy.start())

    def second(j, carry):
        @pl.when(j == 0)
        def _():
            wait_own(1, HIGH)
            fill_own(e2_ref, 1, HIGH, new_disp_ref)

        @pl.when(j == rows - 2 * W)
        def _():
            wait_far(1, HIGH)
            fill_far(e2_ref, 1, HIGH)

        @pl.when(j == rows - W)
        def _():
            wait_own(1, LOW)
            fill_own(e2_ref, 1, LOW, new_disp_ref)
            wait_far(1, LOW)
            fill_far(e2_ref, 1, LOW)

        energy = jnp.zeros(etile_ref.shape, jnp.float32)
        for p in REACH:
            x = lax.rem(j + (W - p + rows), rows)
            parts = {}
            for r in REACH:
                center = [c2_ref[r + W, c, x] for c in range(3)]
                line_energy(p, r, x, center, e2_ref, mask_ref, parts)
            for key, part in parts.items():
                energy = energy + part * jnp.float32(0.25 * math.sqrt(p * p + key))
        etile_ref[...] += energy
        return carry

    lax.fori_loop(0, rows, second, 0)
    def third(x, carry):
        for r in REACH:
            center = [c2_ref[r + W, c, x] for c in range(3)]
            for steps in (REACH[:W], REACH[W:]):
                force = kept_force(r, steps, x, center, e2_ref, mask_ref)
                for c in range(3):
                    force_ref[c, x] += rotated(force[c], -r)
        return carry

    results = [
        pltpu.make_async_copy(acc_ref, acc_hbm, in_sem.at[4]),
        pltpu.make_async_copy(force_ref, force_hbm, in_sem.at[5]),
    ]
    results[0].start()

    def sum_force():
        lax.fori_loop(0, rows, third, 0)
        results[1].start()
        for ex in range(2):
            for g in (HIGH, LOW):
                wait_sent(ex, g)

    moves = []
    if direct:
        me = (ix * ny + iy) * nz + iz
        slots[me] = jnp.sum(etile_ref[...], axis=0, keepdims=True)
        for d in range(1, nx * ny * nz):
            dx, dy, dz = d // (ny * nz), d // nz % ny, d % nz
            copy = pltpu.make_async_remote_copy(
                src_ref=slots.at[me],
                dst_ref=slots.at[me],
                send_sem=esend_sem.at[0],
                recv_sem=erecv_sem.at[0],
                device_id={
                    "gx": lax.rem(ix + dx, nx),
                    "gy": lax.rem(iy + dy, ny),
                    "gz": lax.rem(iz + dz, nz),
                },
                device_id_type=MESH,
            )
            copy.start()
        sum_force()
        landed = slots.at[: nx * ny * nz - 1]
        pltpu.make_async_copy(landed, landed, esend_sem.at[0]).wait()
        pltpu.make_async_copy(landed, landed, erecv_sem.at[0]).wait()
        value = slots[...]
    else:
        sum_force()
        value = jnp.sum(etile_ref[...], axis=0, keepdims=True)
        at = 0
        for axis, count, me in zip(AXES, counts, (ix, iy, iz)):
            base = at + AXES.index(axis)
            slots[base + me] = value
            moves = []
            for d in range(1, count):
                copy = pltpu.make_async_remote_copy(
                    src_ref=slots.at[base + me],
                    dst_ref=slots.at[base + me],
                    send_sem=esend_sem.at[at],
                    recv_sem=erecv_sem.at[at],
                    device_id={axis: lax.rem(me + d, count)},
                    device_id_type=MESH,
                )
                copy.start()
                moves.append(copy)
                at += 1
            for copy in moves:
                copy.wait()
            value = slots[base]
            for i in range(1, count):
                value = value + slots[base + i]
    energy_ref[0, 0] = jnp.sum(value) * jnp.float32(1.0 / area)

    for copy in results:
        copy.wait()


def per_device(displacement, velocity, body_force, broken):
    counts = tuple(lax.axis_size(axis) for axis in AXES)
    _, rows, depth, width = displacement.shape
    area = rows * counts[0] * width * counts[1]
    padded = align(depth + 2 * W)
    slab = align(9 * (rows - W))
    far = align(9 * W)
    devices = math.prod(counts)
    direct = devices if devices <= 64 else 0
    peers = max(direct, sum(counts))
    block = pltpu.VMEM((3, rows, depth, width), jnp.float32)
    out = jax.ShapeDtypeStruct((3, rows, depth, width), jnp.float32)
    hbm = pl.BlockSpec(memory_space=pltpu.HBM)
    span = 2 * W + 1
    e_shape = pltpu.VMEM((span, span, 3, rows + 2 * W, depth, width), jnp.float32)
    turned = pltpu.VMEM((span, 3, rows, depth, width), jnp.float32)
    halo = pltpu.VMEM((3, rows + 2 * W, padded, width), jnp.float32)
    acc, force, energy = pl.pallas_call(
        functools.partial(step_kernel, counts, depth * counts[2], area, direct),
        out_shape=(out, out, jax.ShapeDtypeStruct((1, 1), jnp.float32)),
        in_specs=[hbm] * 4,
        out_specs=(hbm, hbm, pl.BlockSpec(memory_space=pltpu.SMEM)),
        scratch_shapes=[
            block, block, block,
            pltpu.VMEM((broken.shape[0], rows, depth, width), jnp.int32),
            block, block, block,
            e_shape, e_shape, turned, turned, halo, halo,
            pltpu.VMEM((4, padded, width), jnp.float32),
            pltpu.VMEM((len(BONDS), rows, depth, width), jnp.float32),
            pltpu.VMEM((WORD_COUNT, depth, width), jnp.int32),
            pltpu.VMEM((2, 2, 2, slab, width), jnp.float32),
            pltpu.VMEM((2, 2, depth, width), jnp.float32),
            pltpu.VMEM((2, 2, 2, slab + 16, width), jnp.float32),
            pltpu.VMEM((2, 2, 16, width), jnp.float32),
            pltpu.VMEM((2, 2, 2, far + 16, width), jnp.float32),
            pltpu.VMEM((2, 2, 16, width), jnp.float32),
            pltpu.VMEM((2, 2, 3, W, depth, width), jnp.float32),
        ]
        + [
            pltpu.VMEM((max(direct, sum(counts)), 1, width), jnp.float32),
            pltpu.VMEM((depth, width), jnp.float32),
            pltpu.SemaphoreType.DMA((6,)),
            pltpu.SemaphoreType.DMA((2, 2, 7)),
            pltpu.SemaphoreType.DMA((2, 2, 3)),
            pltpu.SemaphoreType.DMA((peers,)),
            pltpu.SemaphoreType.DMA((peers,)),
        ],
        compiler_params=pltpu.CompilerParams(
            collective_id=0, has_side_effects=True, vmem_limit_bytes=67043328
        ),
    )(displacement, velocity, body_force, broken)
    new_displacement = (
        displacement + TIME_STEP * velocity + 0.5 * TIME_STEP * TIME_STEP * acc
    )
    new_acceleration = force + body_force
    new_velocity = velocity + 0.5 * TIME_STEP * (acc + new_acceleration)
    return new_displacement, new_velocity, new_acceleration, energy.reshape(())


def solution(mesh):
    spec = P(None, "gx", "gz", "gy")
    return jax.shard_map(
        per_device,
        mesh=mesh,
        in_specs=(spec,) * 4,
        out_specs=(spec, spec, spec, P()),
        check_vma=False,
    )
```
